16 devices in a mesh: dp: 4 (over z, y), tp: 4 (over x, core).
Axes of the slice: x: 2, y: 2, z: 2, core: 2. Of those that a mesh axis runs over, the one named last changes fastest.
Arguments:
- hidden: bfloat16 [32768, 4096], P(('dp', 'tp')), parts along dimension 0
- norm_gain: float32 [4096], replicated
- w_query: bfloat16 [4096, 32, 128], P(None, 'tp')
- w_key: bfloat16 [4096, 32, 128], P(None, 'tp')
- w_value: bfloat16 [4096, 32, 128], P(None, 'tp')
Outputs:
- output 1: bfloat16 [32768, 32, 128], P('dp', 'tp'), parts along dimension 0
- output 2: bfloat16 [32768, 32, 128], P('dp', 'tp'), parts along dimension 0
- output 3: bfloat16 [32768, 32, 128], P('dp', 'tp'), parts along dimension 0
There are 4 independent parts. The reference program is written for one: setup_inputs(seed, part) draws one part's arguments, and reference() takes and returns one part's arrays. A program takes and returns all parts, laid end to end along the dimension named above; an argument that names none is the same for every part.
All inputs are finite; a program needn't handle non-finite values.
Results may differ from the reference program's by a relative error of at most 0.001.
Values are sent between devices in bfloat16 or wider.
A program may use at most 1 GiB of HBM per device.

```python
import jax
import jax.numpy as jnp
from jax import lax

TOKENS = 8192
MODEL_DIM = 4096
Q_HEADS = 32
KV_COUNT = 32
HEAD_DIM = 128


def setup_inputs(seed: int = 0, part: int = 0) -> dict:
    base_key = jax.random.key(seed)
    part_key = jax.random.fold_in(base_key, part)
    shared = jax.random.split(base_key, 4)
    fan_scale = MODEL_DIM ** -0.5
    hidden = jax.random.normal(part_key, (TOKENS, MODEL_DIM), jnp.float32).astype(jnp.bfloat16)
    norm_gain = jax.random.uniform(shared[0], (MODEL_DIM,), jnp.float32, 0.5, 1.5)
    w_query = (jax.random.normal(shared[1], (MODEL_DIM, Q_HEADS, HEAD_DIM), jnp.float32) * fan_scale).astype(jnp.bfloat16)
    w_key = (jax.random.normal(shared[2], (MODEL_DIM, KV_COUNT, HEAD_DIM), jnp.float32) * fan_scale).astype(jnp.bfloat16)
    w_value = (jax.random.normal(shared[3], (MODEL_DIM, KV_COUNT, HEAD_DIM), jnp.float32) * fan_scale).astype(jnp.bfloat16)
    return {"hidden": hidden, "norm_gain": norm_gain, "w_query": w_query, "w_key": w_key, "w_value": w_value}


def reference(hidden, norm_gain, w_query, w_key, w_value):
    hidden_f32 = hidden.astype(jnp.float32)
    mean_sq = jnp.mean(hidden_f32 * hidden_f32, axis=-1, keepdims=True)
    normed = (hidden_f32 * lax.rsqrt(mean_sq + 1e-6) * norm_gain).astype(jnp.bfloat16)

    def project(weight):
        head_count = weight.shape[1]
        flat_out = jnp.dot(normed, weight.reshape(MODEL_DIM, head_count * HEAD_DIM), preferred_element_type=jnp.float32)
        return flat_out.astype(jnp.bfloat16).reshape(TOKENS, head_count, HEAD_DIM)

    return (project(w_query), project(w_key), project(w_value))
```

```python
import functools

import jax
import jax.numpy as jnp
from jax import lax
from jax.experimental import pallas as pl
from jax.experimental.pallas import tpu as pltpu
from jax.sharding import PartitionSpec as P


HEADS = 8
HEAD_DIM = 128
COLS = HEADS * HEAD_DIM
MIB = 1024 * 1024
VMEM = 60 * MIB
PROJECT_VMEM = 42 * MIB

CHUNKS = (256, 256, 256, 256, 256, 256, 256, 128, 128)
BIG = 512


def normalize(x, norm_gain, start, rows, step):
    dim = x.shape[1]

    def body(x_ref, g_ref, n_ref):
        def piece(i, carry):
            at = pl.ds(pl.multiple_of(i * 16, 16), 16)
            v = x_ref[at, :].astype(jnp.float32)
            scale = lax.rsqrt(jnp.mean(v * v, axis=-1, keepdims=True) + 1e-6)
            n_ref[at, :] = (v * scale * g_ref[...]).astype(jnp.bfloat16)
            return carry

        lax.fori_loop(0, step // 16, piece, 0)

    return pl.pallas_call(
        body,
        grid=(rows // step,),
        in_specs=[
            pl.BlockSpec((step, dim), lambda i: (start // step + i, 0)),
            pl.BlockSpec((1, dim), lambda i: (0, 0)),
        ],
        out_specs=pl.BlockSpec((step, dim), lambda i: (i, 0)),
        out_shape=jax.ShapeDtypeStruct((rows, dim), jnp.bfloat16),
        compiler_params=pltpu.CompilerParams(vmem_limit_bytes=VMEM),
        cost_estimate=pl.CostEstimate(flops=8 * rows * dim, bytes_accessed=4 * rows * dim, transcendentals=rows),
        name="normalize",
    )(x, norm_gain.reshape(1, dim))


def join_weights(*weights):
    dim = weights[0].shape[0]
    step = 256

    def body(a_ref, b_ref, c_ref, w_ref, flat):
        for index, ref in enumerate((a_ref, b_ref, c_ref)):
            flat[...] = ref[...].astype(jnp.float32).reshape(step * HEADS, HEAD_DIM)
            for head in range(HEADS):
                part = flat[pl.ds(head, step, stride=HEADS), :]
                w_ref[index, :, head * HEAD_DIM : (head + 1) * HEAD_DIM] = part.astype(jnp.bfloat16)

    return pl.pallas_call(
        body,
        grid=(dim // step,),
        in_specs=[pl.BlockSpec((step, HEADS, HEAD_DIM), lambda i: (i, 0, 0))] * 3,
        out_specs=pl.BlockSpec((3, step, COLS), lambda i: (0, i, 0)),
        out_shape=jax.ShapeDtypeStruct((3, dim, COLS), jnp.bfloat16),
        scratch_shapes=[pltpu.VMEM((step * HEADS, HEAD_DIM), jnp.float32)],
        compiler_params=pltpu.CompilerParams(vmem_limit_bytes=VMEM),
        cost_estimate=pl.CostEstimate(flops=6 * dim * COLS, bytes_accessed=12 * dim * COLS, transcendentals=0),
        name="join_weights",
    )(*weights)


def product(n_ref, w_ref, total):
    rows = n_ref.shape[0]

    def pair(i, carry):
        cols = pl.ds(pl.multiple_of(i * 2 * HEAD_DIM, 2 * HEAD_DIM), 2 * HEAD_DIM)
        part = jnp.dot(n_ref[...], w_ref[0, :, cols], preferred_element_type=jnp.float32)
        for side in range(2):
            total[pl.ds(2 * i + side, rows, stride=HEADS), :] = part[:, side * HEAD_DIM : (side + 1) * HEAD_DIM]
        return carry

    lax.fori_loop(0, HEADS // 2, pair, 0)


def emit(total, out_ref):
    rows = out_ref.shape[0]
    step = 32

    def piece(i, carry):
        src = pl.ds(pl.multiple_of(i * step * HEADS, step * HEADS), step * HEADS)
        dst = pl.ds(pl.multiple_of(i * step, step), step)
        out_ref[dst] = total[src, :].reshape(step, HEADS, HEAD_DIM).astype(out_ref.dtype)
        return carry

    lax.fori_loop(0, rows // step, piece, 0)


def project(n, w, owners, which, outs, tokens):
    rows, dim = n.shape
    blocks = rows // BIG

    def body(owners_ref, n_ref, w_ref, *refs):
        q_ref, k_ref, v_ref, total = refs[-4:]
        product(n_ref, w_ref, total)
        j = pl.program_id(1)
        for index, out_ref in enumerate((q_ref, k_ref, v_ref)):
            pl.when(j == index)(functools.partial(emit, total, out_ref))

    out_spec = pl.BlockSpec((BIG, HEADS, HEAD_DIM), lambda r, j, owners: (owners[which] * blocks + r, 0, 0))
    return pl.pallas_call(
        body,
        grid_spec=pltpu.PrefetchScalarGridSpec(
            num_scalar_prefetch=1,
            grid=(blocks, 3),
            in_specs=[
                pl.BlockSpec((BIG, dim), lambda r, j, owners: (r, 0)),
                pl.BlockSpec((1, dim, COLS), lambda r, j, owners: (j, 0, 0)),
            ]
            + [pl.BlockSpec(memory_space=pl.ANY)] * len(outs),
            out_specs=[out_spec] * 3,
            scratch_shapes=[pltpu.VMEM((BIG * HEADS, HEAD_DIM), jnp.float32)],
        ),
        out_shape=[jax.ShapeDtypeStruct((tokens, HEADS, HEAD_DIM), jnp.bfloat16)] * 3,
        input_output_aliases={3 + i: i for i in range(len(outs))},
        compiler_params=pltpu.CompilerParams(vmem_limit_bytes=PROJECT_VMEM),
        cost_estimate=pl.CostEstimate(
            flops=6 * rows * dim * COLS,
            bytes_accessed=2 * (rows * dim + 3 * blocks * dim * COLS + 3 * rows * COLS),
            transcendentals=0,
        ),
        name="project",
    )(owners, n, w, *outs)


def project_two(near, far, w, owners, start, block, outs, tokens):
    rows, dim = near.shape

    def body(owners_ref, near_ref, far_ref, w_ref, *refs):
        q_ref, k_ref, v_ref, total = refs[-4:]
        j, r = pl.program_id(0), pl.program_id(1)
        for index, n_ref in enumerate((near_ref, far_ref)):
            pl.when(r == index)(functools.partial(product, n_ref, w_ref, total))
        for index, out_ref in enumerate((q_ref, k_ref, v_ref)):
            pl.when(j == index)(functools.partial(emit, total, out_ref))

    def out_spec(index):
        def at_step(j, r, owners):
            side = jnp.where(j < index, 0, jnp.where(j > index, 1, r))
            return (owners[2 + side] * (block // rows) + start // rows, 0, 0)

        return pl.BlockSpec((rows, HEADS, HEAD_DIM), at_step)

    whole = pl.BlockSpec((rows, dim), lambda j, r, owners: (0, 0))
    return pl.pallas_call(
        body,
        grid_spec=pltpu.PrefetchScalarGridSpec(
            num_scalar_prefetch=1,
            grid=(3, 2),
            in_specs=[whole, whole, pl.BlockSpec((1, dim, COLS), lambda j, r, owners: (j, 0, 0))]
            + [pl.BlockSpec(memory_space=pl.ANY)] * 3,
            out_specs=[out_spec(i) for i in range(3)],
            scratch_shapes=[pltpu.VMEM((rows * HEADS, HEAD_DIM), jnp.float32)],
        ),
        out_shape=[jax.ShapeDtypeStruct((tokens, HEADS, HEAD_DIM), jnp.bfloat16)] * 3,
        input_output_aliases={4 + i: i for i in range(3)},
        compiler_params=pltpu.CompilerParams(vmem_limit_bytes=PROJECT_VMEM),
        cost_estimate=pl.CostEstimate(
            flops=12 * rows * dim * COLS,
            bytes_accessed=2 * (2 * rows * dim + 3 * dim * COLS + 6 * rows * COLS),
            transcendentals=0,
        ),
        name="project_two",
    )(owners, near, far, w, *outs)


def solution(mesh):
    across = [(0, 2), (1, 3), (2, 0), (3, 1)]
    beside = [(0, 1), (1, 0), (2, 3), (3, 2)]

    def inner(hidden_blk, norm_gain, wq_local, wk_local, wv_local):
        block, _ = hidden_blk.shape
        tokens = 4 * block
        me = lax.axis_index("tp").astype(jnp.int32)
        owners = me ^ jnp.arange(4, dtype=jnp.int32)
        starts = [sum(CHUNKS[:i]) for i in range(len(CHUNKS))]

        x, near = hidden_blk, []
        for s, c in zip(starts, CHUNKS):
            mine = normalize(x, norm_gain, s, c, 128)
            x, mine = lax.optimization_barrier((x, mine))
            near.append(lax.ppermute(mine, "tp", across))
        own = normalize(x, norm_gain, 0, block, 128)
        paired = lax.ppermute(own, "tp", beside)
        w = join_weights(wq_local, wk_local, wv_local)

        far = {}

        def arrive(outs, *chunks):
            got = lax.optimization_barrier((tuple(near[i] for i in chunks), tuple(outs)))
            for i, a in zip(chunks, got[0]):
                near[i] = a
                far[i] = lax.ppermute(a, "tp", beside)
            return got[1]

        outs = project(own, w, owners, 0, (), tokens)
        outs = arrive(outs, 0, 1)
        outs = project(paired, w, owners, 1, outs, tokens)
        outs = arrive(outs, 2)
        after = {0: 3, 3: 4}
        for i, (s, c) in enumerate(zip(starts, CHUNKS)):
            if i > 4:
                outs = arrive(outs, i)
            outs = project_two(near[i], far[i], w, owners, s, block, outs, tokens)
            if i in after:
                outs = arrive(outs, after[i])
        return tuple(outs)

    row_spec = P(("dp", "tp"), None)
    head_spec = P(None, "tp", None)
    out_spec = P("dp", "tp", None)
    return jax.shard_map(inner, mesh=mesh, in_specs=(row_spec, P(None), head_spec, head_spec, head_spec), out_specs=(out_spec, out_spec, out_spec), check_vma=False)
```

```python
import jax
import jax.numpy as jnp
from jax import lax
from jax.experimental import pallas as pl
from jax.experimental.pallas import tpu as pltpu
from jax.sharding import PartitionSpec as P


HEADS = 8
HEAD_DIM = 128
COLS = HEADS * HEAD_DIM
PIECE = 2 * HEAD_DIM
PIECES = COLS // PIECE
RING = 6
MIB = 1024 * 1024
VMEM = 60 * MIB
PROJECT_VMEM = 42 * MIB

CHUNKS = (256, 256, 256, 256, 256, 256, 256, 128, 128)
BIG = 512
NORM_ROWS = 128


def normalize_rows(x_ref, g_ref, n_ref):
    def piece(i, carry):
        at = pl.ds(pl.multiple_of(i * 32, 32), 32)
        v = x_ref[at, :].astype(jnp.float32)
        scale = lax.rsqrt(jnp.mean(v * v, axis=-1, keepdims=True) + 1e-6)
        n_ref[at, :] = (v * scale * g_ref[...]).astype(jnp.bfloat16)
        return carry

    lax.fori_loop(0, x_ref.shape[0] // 32, piece, 0)


def normalize_first(x, norm_gain, rows):
    dim = x.shape[1]
    step = 64
    return pl.pallas_call(
        normalize_rows,
        grid=(rows // step,),
        in_specs=[pl.BlockSpec((step, dim), lambda i: (i, 0)), pl.BlockSpec((1, dim), lambda i: (0, 0))],
        out_specs=pl.BlockSpec((step, dim), lambda i: (i, 0)),
        out_shape=jax.ShapeDtypeStruct((rows, dim), jnp.bfloat16),
        compiler_params=pltpu.CompilerParams(vmem_limit_bytes=VMEM),
        cost_estimate=pl.CostEstimate(flops=8 * rows * dim, bytes_accessed=4 * rows * dim, transcendentals=rows),
        name="normalize_first",
    )(x, norm_gain)


def normalize_all(x, norm_gain, chunks):
    block, dim = x.shape
    step = NORM_ROWS
    bounds = [sum(chunks[:i]) // step for i in range(len(chunks) + 1)]

    def body(x_ref, g_ref, *refs):
        outs, (held, sem) = refs[:-2], refs[-2:]
        b = pl.program_id(0)
        slot = lax.rem(b, 2)

        def copies(b, slot, do):
            do(pltpu.make_async_copy(held.at[slot], outs[0].at[pl.ds(b * step, step)], sem.at[slot, 0]))
            for i in range(1, len(chunks)):

                @pl.when((b >= bounds[i]) & (b < bounds[i + 1]))
                def _(i=i):
                    to = outs[i].at[pl.ds((b - bounds[i]) * step, step)]
                    do(pltpu.make_async_copy(held.at[slot], to, sem.at[slot, 1]))

        pl.when(b >= 2)(lambda: copies(b - 2, slot, lambda c: c.wait()))
        normalize_rows(x_ref, g_ref, held.at[slot])
        copies(b, slot, lambda c: c.start())

        @pl.when(b == block // step - 1)
        def _():
            copies(b - 1, 1 - slot, lambda c: c.wait())
            copies(b, slot, lambda c: c.wait())

    return pl.pallas_call(
        body,
        grid=(block // step,),
        in_specs=[pl.BlockSpec((step, dim), lambda i: (i, 0)), pl.BlockSpec((1, dim), lambda i: (0, 0))],
        out_specs=[pl.BlockSpec(memory_space=pl.ANY)] * len(chunks),
        out_shape=[jax.ShapeDtypeStruct((rows, dim), jnp.bfloat16) for rows in (block,) + chunks[1:]],
        scratch_shapes=[pltpu.VMEM((2, step, dim), jnp.bfloat16), pltpu.SemaphoreType.DMA((2, 2))],
        compiler_params=pltpu.CompilerParams(vmem_limit_bytes=VMEM),
        cost_estimate=pl.CostEstimate(flops=8 * block * dim, bytes_accessed=6 * block * dim, transcendentals=block),
        name="normalize_all",
    )(x, norm_gain)


def join_weights(*weights):
    dim = weights[0].shape[0]
    step, sub = 256, 64

    def body(a_ref, b_ref, c_ref, w_ref, flat):
        def some(i, carry):
            at = pl.ds(pl.multiple_of(i * sub, sub), sub)
            for index, ref in enumerate((a_ref, b_ref, c_ref)):
                flat[index] = ref[at].astype(jnp.float32).reshape(sub * HEADS, HEAD_DIM)
            for index in range(3):
                for head in range(HEADS):
                    part = flat[index, pl.ds(head, sub, stride=HEADS), :]
                    lanes = slice(head % 2 * HEAD_DIM, (head % 2 + 1) * HEAD_DIM)
                    w_ref[index * PIECES + head // 2, at, lanes] = part.astype(jnp.bfloat16)
            return carry

        lax.fori_loop(0, step // sub, some, 0)

    return pl.pallas_call(
        body,
        grid=(dim // step,),
        in_specs=[pl.BlockSpec((step, HEADS, HEAD_DIM), lambda i: (i, 0, 0))] * 3,
        out_specs=pl.BlockSpec((3 * PIECES, step, PIECE), lambda i: (0, i, 0)),
        out_shape=jax.ShapeDtypeStruct((3 * PIECES, dim, PIECE), jnp.bfloat16),
        scratch_shapes=[pltpu.VMEM((3, sub * HEADS, HEAD_DIM), jnp.float32)],
        compiler_params=pltpu.CompilerParams(vmem_limit_bytes=VMEM),
        cost_estimate=pl.CostEstimate(flops=6 * dim * COLS, bytes_accessed=12 * dim * COLS, transcendentals=0),
        name="join_weights",
    )(*weights)


def project(parts, w, owners, outs, tokens):
    arrays = [p[0] for p in parts]
    dim = w.shape[1]
    sizes = [p[1] for p in parts]
    offsets = [sum(sizes[:i]) for i in range(len(sizes))]
    rows = sum(sizes)
    blocks = arrays[0].shape[0] // sizes[0]
    steps = 3 * blocks
    slots = min(blocks, 2)
    quarter = rows // PIECES

    def body(owners_ref, *refs):
        n_hbm, w_hbm = refs[: len(parts)], refs[len(parts)]
        q_out, k_out, v_out, n_buf, w_buf, total, stage, n_sem, w_sem, o_sem = refs[-10:]

        def fetch(b, do):
            slot = lax.rem(b, slots)
            for i, size in enumerate(sizes):
                src = n_hbm[i].at[pl.ds(pl.multiple_of(b * size, size), size)]
                do(pltpu.make_async_copy(src, n_buf.at[slot, pl.ds(offsets[i], size)], n_sem.at[slot, i]))

        def piece(p, do):
            slot = lax.rem(p, RING)
            do(pltpu.make_async_copy(w_hbm.at[lax.rem(p, 3 * PIECES)], w_buf.at[slot], w_sem.at[slot]))

        def store(s, do):
            b, j = s // 3, lax.rem(s, 3)
            slot = lax.rem(s, 2)
            for index, out in enumerate((q_out, k_out, v_out)):

                @pl.when(j == index)
                def _(out=out):
                    for i, (_, size, which, start) in enumerate(parts):
                        first = owners_ref[which] * (tokens // 4) + start + b * size
                        src = stage.at[slot, pl.ds(offsets[i], size)]
                        do(pltpu.make_async_copy(src, out.at[pl.ds(first, size)], o_sem.at[slot, i]))

        def emit(slot, start, size):
            src = pl.ds(pl.multiple_of(start * HEADS, size * HEADS), size * HEADS)
            got = total[slot, src, :].reshape(size, HEADS, HEAD_DIM).astype(jnp.bfloat16)
            stage[slot, pl.ds(pl.multiple_of(start, size), size)] = got

        def begin(copy):
            copy.start()

        def end(copy):
            copy.wait()

        fetch(0, begin)
        for p in range(RING - 1):
            piece(p, begin)

        def step(s, carry):
            b, j = s // 3, lax.rem(s, 3)
            slot = lax.rem(s, 2)
            pl.when(s >= 3)(lambda: store(s - 3, end))

            @pl.when(j == 0)
            def _():
                fetch(b, end)
                if blocks > 1:
                    pl.when(b + 1 < blocks)(lambda: fetch(b + 1, begin))

            def part(i, carry):
                p = s * PIECES + i
                piece(p, end)
                pl.when(p + RING - 1 < steps * PIECES)(lambda: piece(p + RING - 1, begin))
                emit(1 - slot, i * quarter, quarter)
                got = jnp.dot(n_buf[lax.rem(b, slots)], w_buf[lax.rem(p, RING)], preferred_element_type=jnp.float32)
                for side in range(2):
                    total[slot, pl.ds(2 * i + side, rows, stride=HEADS), :] = got[:, side * HEAD_DIM : (side + 1) * HEAD_DIM]
                return carry

            lax.fori_loop(0, PIECES, part, 0)
            pl.when(s >= 1)(lambda: store(s - 1, begin))
            return carry

        lax.fori_loop(0, steps, step, 0)
        last = steps - 1
        store(last - 2, end)
        lax.fori_loop(0, PIECES, lambda i, carry: (emit(last % 2, i * quarter, quarter), carry)[1], 0)
        store(last, begin)
        store(last - 1, end)
        store(last, end)

    return pl.pallas_call(
        body,
        in_specs=[pl.BlockSpec(memory_space=pltpu.SMEM)] + [pl.BlockSpec(memory_space=pltpu.HBM)] * (len(parts) + 1 + len(outs)),
        out_specs=[pl.BlockSpec(memory_space=pl.ANY)] * 3,
        out_shape=[jax.ShapeDtypeStruct((tokens, HEADS, HEAD_DIM), jnp.bfloat16)] * 3,
        scratch_shapes=[
            pltpu.VMEM((slots, rows, dim), jnp.bfloat16),
            pltpu.VMEM((RING, dim, PIECE), jnp.bfloat16),
            pltpu.VMEM((2, rows * HEADS, HEAD_DIM), jnp.float32),
            pltpu.VMEM((2, rows, HEADS, HEAD_DIM), jnp.bfloat16),
            pltpu.SemaphoreType.DMA((slots, len(parts))),
            pltpu.SemaphoreType.DMA((RING,)),
            pltpu.SemaphoreType.DMA((2, len(parts))),
        ],
        input_output_aliases={len(parts) + 2 + i: i for i in range(len(outs))},
        compiler_params=pltpu.CompilerParams(vmem_limit_bytes=PROJECT_VMEM),
        cost_estimate=pl.CostEstimate(
            flops=6 * blocks * rows * dim * COLS,
            bytes_accessed=2 * blocks * (rows * dim + 3 * dim * COLS + 3 * rows * COLS),
            transcendentals=0,
        ),
        name="project",
    )(owners, *arrays, w, *outs)


def solution(mesh):
    across = [(0, 2), (1, 3), (2, 0), (3, 1)]
    beside = [(0, 1), (1, 0), (2, 3), (3, 2)]

    def inner(hidden_blk, norm_gain, wq_local, wk_local, wv_local):
        block, dim = hidden_blk.shape
        tokens = 4 * block
        me = lax.axis_index("tp").astype(jnp.int32)
        owners = me ^ jnp.arange(4, dtype=jnp.int32)
        starts = [sum(CHUNKS[:i]) for i in range(len(CHUNKS))]

        gain = norm_gain.reshape(1, dim)
        mine = [normalize_first(hidden_blk, gain, CHUNKS[0])]
        near = [lax.ppermute(mine[0], "tp", across)]
        own, *rest = normalize_all(hidden_blk, gain, CHUNKS)
        for m in rest:
            near.append(lax.ppermute(m, "tp", across))
        paired = lax.ppermute(own, "tp", beside)
        w = join_weights(wq_local, wk_local, wv_local)

        far = {}

        def arrive(outs, *chunks):
            got = lax.optimization_barrier((tuple(near[i] for i in chunks), tuple(outs)))
            for i, a in zip(chunks, got[0]):
                near[i] = a
                far[i] = lax.ppermute(a, "tp", beside)
            return got[1]

        outs = project([(own, BIG, 0, 0)], w, owners, (), tokens)
        outs = arrive(outs, 0, 1)
        outs = project([(paired, BIG, 1, 0)], w, owners, outs, tokens)
        outs = arrive(outs, 2)
        after = {1: 3, 3: 4}
        for i, (s, c) in enumerate(zip(starts, CHUNKS)):
            if i > 4:
                outs = arrive(outs, i)
            outs = project([(near[i], c, 2, s), (far[i], c, 3, s)], w, owners, outs, tokens)
            if i in after:
                outs = arrive(outs, after[i])
        return tuple(outs)

    row_spec = P(("dp", "tp"), None)
    head_spec = P(None, "tp", None)
    out_spec = P("dp", "tp", None)
    return jax.shard_map(inner, mesh=mesh, in_specs=(row_spec, P(None), head_spec, head_spec, head_spec), out_specs=(out_spec, out_spec, out_spec), check_vma=False)
```

```python
import jax
import jax.numpy as jnp
from jax import lax
from jax.experimental import pallas as pl
from jax.experimental.pallas import tpu as pltpu
from jax.sharding import PartitionSpec as P


HEADS = 8
HEAD_DIM = 128
COLS = HEADS * HEAD_DIM
SIDES = 4
PIECE = SIDES * HEAD_DIM
PIECES = COLS // PIECE
RING = 4
MIB = 1024 * 1024
VMEM = 60 * MIB
PROJECT_VMEM = 42 * MIB

CHUNKS = (256, 256, 256, 256, 256, 256, 256, 128, 128)
BIG = 512
NORM_ROWS = 128


def normalize_rows(x_ref, g_ref, n_ref):
    sub, lanes = 32, 128
    dim = x_ref.shape[1]

    def piece(i, carry):
        at = pl.ds(pl.multiple_of(i * sub, sub), sub)
        squares = [jnp.zeros((sub, lanes), jnp.float32) for _ in range(2)]
        for k in range(dim // lanes):
            v = x_ref[at, k * lanes : (k + 1) * lanes].astype(jnp.float32)
            squares[k % 2] += v * v
        mean = jnp.sum(squares[0] + squares[1], axis=-1, keepdims=True) / dim
        scale = jnp.broadcast_to(lax.rsqrt(mean + 1e-6), (sub, lanes))
        for k in range(dim // lanes):
            cols = slice(k * lanes, (k + 1) * lanes)
            n_ref[at, cols] = (x_ref[at, cols].astype(jnp.float32) * scale * g_ref[:, cols]).astype(jnp.bfloat16)
        return carry

    lax.fori_loop(0, x_ref.shape[0] // sub, piece, 0)


def normalize_first(x, norm_gain, rows):
    dim = x.shape[1]
    step = 64
    return pl.pallas_call(
        normalize_rows,
        grid=(rows // step,),
        in_specs=[pl.BlockSpec((step, dim), lambda i: (i, 0)), pl.BlockSpec((1, dim), lambda i: (0, 0))],
        out_specs=pl.BlockSpec((step, dim), lambda i: (i, 0)),
        out_shape=jax.ShapeDtypeStruct((rows, dim), jnp.bfloat16),
        compiler_params=pltpu.CompilerParams(vmem_limit_bytes=VMEM),
        cost_estimate=pl.CostEstimate(flops=8 * rows * dim, bytes_accessed=4 * rows * dim, transcendentals=rows),
        name="normalize_first",
    )(x, norm_gain)


def normalize_all(x, norm_gain, chunks):
    block, dim = x.shape
    step = NORM_ROWS
    bounds = [sum(chunks[:i]) // step for i in range(len(chunks) + 1)]

    def body(x_ref, g_ref, *refs):
        outs, (held, sem) = refs[:-2], refs[-2:]
        b = pl.program_id(0)
        slot = lax.rem(b, 2)

        def copies(b, slot, do):
            do(pltpu.make_async_copy(held.at[slot], outs[0].at[pl.ds(b * step, step)], sem.at[slot, 0]))
            for i in range(1, len(chunks)):

                @pl.when((b >= bounds[i]) & (b < bounds[i + 1]))
                def _(i=i):
                    to = outs[i].at[pl.ds((b - bounds[i]) * step, step)]
                    do(pltpu.make_async_copy(held.at[slot], to, sem.at[slot, 1]))

        pl.when(b >= 2)(lambda: copies(b - 2, slot, lambda c: c.wait()))
        normalize_rows(x_ref, g_ref, held.at[slot])
        copies(b, slot, lambda c: c.start())

        @pl.when(b == block // step - 1)
        def _():
            copies(b - 1, 1 - slot, lambda c: c.wait())
            copies(b, slot, lambda c: c.wait())

    return pl.pallas_call(
        body,
        grid=(block // step,),
        in_specs=[pl.BlockSpec((step, dim), lambda i: (i, 0)), pl.BlockSpec((1, dim), lambda i: (0, 0))],
        out_specs=[pl.BlockSpec(memory_space=pl.ANY)] * len(chunks),
        out_shape=[jax.ShapeDtypeStruct((rows, dim), jnp.bfloat16) for rows in (block,) + chunks[1:]],
        scratch_shapes=[pltpu.VMEM((2, step, dim), jnp.bfloat16), pltpu.SemaphoreType.DMA((2, 2))],
        compiler_params=pltpu.CompilerParams(vmem_limit_bytes=VMEM),
        cost_estimate=pl.CostEstimate(flops=8 * block * dim, bytes_accessed=6 * block * dim, transcendentals=block),
        name="normalize_all",
    )(x, norm_gain)


def join_weights(*weights):
    dim = weights[0].shape[0]
    step, sub = 512, 64

    def body(a_ref, b_ref, c_ref, w_ref, flat):
        def some(i, carry):
            at = pl.ds(pl.multiple_of(i * sub, sub), sub)
            for index, ref in enumerate((a_ref, b_ref, c_ref)):
                flat[index] = ref[at].astype(jnp.float32).reshape(sub * HEADS, HEAD_DIM)
            for index in range(3):
                for head in range(HEADS):
                    part = flat[index, pl.ds(head, sub, stride=HEADS), :]
                    lanes = slice(head % SIDES * HEAD_DIM, (head % SIDES + 1) * HEAD_DIM)
                    w_ref[index * PIECES + head // SIDES, at, lanes] = part.astype(jnp.bfloat16)
            return carry

        lax.fori_loop(0, step // sub, some, 0)

    return pl.pallas_call(
        body,
        grid=(dim // step,),
        in_specs=[pl.BlockSpec((step, HEADS, HEAD_DIM), lambda i: (i, 0, 0))] * 3,
        out_specs=pl.BlockSpec((3 * PIECES, step, PIECE), lambda i: (0, i, 0)),
        out_shape=jax.ShapeDtypeStruct((3 * PIECES, dim, PIECE), jnp.bfloat16),
        scratch_shapes=[pltpu.VMEM((3, sub * HEADS, HEAD_DIM), jnp.float32)],
        compiler_params=pltpu.CompilerParams(vmem_limit_bytes=VMEM),
        cost_estimate=pl.CostEstimate(flops=6 * dim * COLS, bytes_accessed=12 * dim * COLS, transcendentals=0),
        name="join_weights",
    )(*weights)


def project(parts, w, owners, outs, tokens):
    arrays = [p[0] for p in parts]
    dim = w.shape[1]
    sizes = [p[1] for p in parts]
    offsets = [sum(sizes[:i]) for i in range(len(sizes))]
    rows = sum(sizes)
    blocks = arrays[0].shape[0] // sizes[0]
    steps = 3 * blocks
    slots = min(blocks, 2)
    quarter = rows // PIECES

    def body(owners_ref, *refs):
        n_hbm, w_hbm = refs[: len(parts)], refs[len(parts)]
        q_out, k_out, v_out, n_buf, w_buf, total, stage, n_sem, w_sem, o_sem = refs[-10:]

        def fetch(b, do):
            slot = lax.rem(b, slots)
            for i, size in enumerate(sizes):
                src = n_hbm[i].at[pl.ds(pl.multiple_of(b * size, size), size)]
                do(pltpu.make_async_copy(src, n_buf.at[slot, pl.ds(offsets[i], size)], n_sem.at[slot, i]))

        def piece(p, do):
            slot = lax.rem(p, RING)
            do(pltpu.make_async_copy(w_hbm.at[lax.rem(p, 3 * PIECES)], w_buf.at[slot], w_sem.at[slot]))

        def store(s, do):
            b, j = s // 3, lax.rem(s, 3)
            slot = lax.rem(s, 2)
            for index, out in enumerate((q_out, k_out, v_out)):

                @pl.when(j == index)
                def _(out=out):
                    for i, (_, size, which, start) in enumerate(parts):
                        first = owners_ref[which] * (tokens // 4) + start + b * size
                        src = stage.at[slot, pl.ds(offsets[i], size)]
                        do(pltpu.make_async_copy(src, out.at[pl.ds(first, size)], o_sem.at[slot, i]))

        def emit(slot, start, size):
            src = pl.ds(pl.multiple_of(start * HEADS, size * HEADS), size * HEADS)
            got = total[slot, src, :].reshape(size, HEADS, HEAD_DIM).astype(jnp.bfloat16)
            stage[slot, pl.ds(pl.multiple_of(start, size), size)] = got

        def begin(copy):
            copy.start()

        def end(copy):
            copy.wait()

        fetch(0, begin)
        for p in range(RING - 1):
            piece(p, begin)

        def step(s, carry):
            b, j = s // 3, lax.rem(s, 3)
            slot = lax.rem(s, 2)
            pl.when(s >= 3)(lambda: store(s - 3, end))

            @pl.when(j == 0)
            def _():
                fetch(b, end)
                if blocks > 1:
                    pl.when(b + 1 < blocks)(lambda: fetch(b + 1, begin))

            def part(i, carry):
                p = s * PIECES + i
                piece(p, end)
                pl.when(p + RING - 1 < steps * PIECES)(lambda: piece(p + RING - 1, begin))
                emit(1 - slot, i * quarter, quarter)
                got = jnp.dot(n_buf[lax.rem(b, slots)], w_buf[lax.rem(p, RING)], preferred_element_type=jnp.float32)
                for side in range(SIDES):
                    total[slot, pl.ds(SIDES * i + side, rows, stride=HEADS), :] = got[:, side * HEAD_DIM : (side + 1) * HEAD_DIM]
                return carry

            lax.fori_loop(0, PIECES, part, 0)
            pl.when(s >= 1)(lambda: store(s - 1, begin))
            return carry

        lax.fori_loop(0, steps, step, 0)
        last = steps - 1
        store(last - 2, end)
        lax.fori_loop(0, PIECES, lambda i, carry: (emit(last % 2, i * quarter, quarter), carry)[1], 0)
        store(last, begin)
        store(last - 1, end)
        store(last, end)

    return pl.pallas_call(
        body,
        in_specs=[pl.BlockSpec(memory_space=pltpu.SMEM)] + [pl.BlockSpec(memory_space=pltpu.HBM)] * (len(parts) + 1 + len(outs)),
        out_specs=[pl.BlockSpec(memory_space=pl.ANY)] * 3,
        out_shape=[jax.ShapeDtypeStruct((tokens, HEADS, HEAD_DIM), jnp.bfloat16)] * 3,
        scratch_shapes=[
            pltpu.VMEM((slots, rows, dim), jnp.bfloat16),
            pltpu.VMEM((RING, dim, PIECE), jnp.bfloat16),
            pltpu.VMEM((2, rows * HEADS, HEAD_DIM), jnp.float32),
            pltpu.VMEM((2, rows, HEADS, HEAD_DIM), jnp.bfloat16),
            pltpu.SemaphoreType.DMA((slots, len(parts))),
            pltpu.SemaphoreType.DMA((RING,)),
            pltpu.SemaphoreType.DMA((2, len(parts))),
        ],
        input_output_aliases={len(parts) + 2 + i: i for i in range(len(outs))},
        compiler_params=pltpu.CompilerParams(vmem_limit_bytes=PROJECT_VMEM),
        cost_estimate=pl.CostEstimate(
            flops=6 * blocks * rows * dim * COLS,
            bytes_accessed=2 * blocks * (rows * dim + 3 * dim * COLS + 3 * rows * COLS),
            transcendentals=0,
        ),
        name="project",
    )(owners, *arrays, w, *outs)


def solution(mesh):
    across = [(0, 2), (1, 3), (2, 0), (3, 1)]
    beside = [(0, 1), (1, 0), (2, 3), (3, 2)]

    def inner(hidden_blk, norm_gain, wq_local, wk_local, wv_local):
        block, dim = hidden_blk.shape
        tokens = 4 * block
        me = lax.axis_index("tp").astype(jnp.int32)
        owners = me ^ jnp.arange(4, dtype=jnp.int32)
        starts = [sum(CHUNKS[:i]) for i in range(len(CHUNKS))]

        gain = norm_gain.reshape(1, dim)
        mine = [normalize_first(hidden_blk, gain, CHUNKS[0])]
        near = [lax.ppermute(mine[0], "tp", across)]
        own, *rest = normalize_all(hidden_blk, gain, CHUNKS)
        for m in rest:
            near.append(lax.ppermute(m, "tp", across))
        paired = lax.ppermute(own, "tp", beside)
        w = join_weights(wq_local, wk_local, wv_local)

        far = {}

        def arrive(outs, *chunks):
            got = lax.optimization_barrier((tuple(near[i] for i in chunks), tuple(outs)))
            for i, a in zip(chunks, got[0]):
                near[i] = a
                far[i] = lax.ppermute(a, "tp", beside)
            return got[1]

        outs = project([(own, BIG, 0, 0)], w, owners, (), tokens)
        outs = arrive(outs, 0, 1)
        outs = project([(paired, BIG, 1, 0)], w, owners, outs, tokens)
        outs = arrive(outs, 2)
        after = {1: 3, 3: 4}
        for i, (s, c) in enumerate(zip(starts, CHUNKS)):
            if i > 4:
                outs = arrive(outs, i)
            outs = project([(near[i], c, 2, s), (far[i], c, 3, s)], w, owners, outs, tokens)
            if i in after:
                outs = arrive(outs, after[i])
        return tuple(outs)

    row_spec = P(("dp", "tp"), None)
    head_spec = P(None, "tp", None)
    out_spec = P("dp", "tp", None)
    return jax.shard_map(inner, mesh=mesh, in_specs=(row_spec, P(None), head_spec, head_spec, head_spec), out_specs=(out_spec, out_spec, out_spec), check_vma=False)
```

```python
import jax
import jax.numpy as jnp
from jax import lax
from jax.experimental import pallas as pl
from jax.experimental.pallas import tpu as pltpu
from jax.sharding import PartitionSpec as P


HEADS = 8
HEAD_DIM = 128
COLS = HEADS * HEAD_DIM
SIDES = 4
PIECE = SIDES * HEAD_DIM
PIECES = COLS // PIECE
MIB = 1024 * 1024
VMEM = 60 * MIB
PROJECT_VMEM = 24 * MIB
JOIN_VMEM = 24 * MIB

CHUNKS = (64, 192, 256, 256, 256, 256, 256, 256, 128, 96, 32)
EARLY = 2
BIG = 512
NORM_ROWS = 128


def normalize_rows(x_ref, g_ref, n_ref):
    sub, lanes = 32, 128
    dim = x_ref.shape[1]

    def piece(i, carry):
        at = pl.ds(pl.multiple_of(i * sub, sub), sub)
        squares = [jnp.zeros((sub, lanes), jnp.float32) for _ in range(2)]
        for k in range(dim // lanes):
            v = x_ref[at, k * lanes : (k + 1) * lanes].astype(jnp.float32)
            squares[k % 2] += v * v
        mean = jnp.sum(squares[0] + squares[1], axis=-1, keepdims=True) / dim
        scale = jnp.broadcast_to(lax.rsqrt(mean + 1e-6), (sub, lanes))
        for k in range(dim // lanes):
            cols = slice(k * lanes, (k + 1) * lanes)
            n_ref[at, cols] = (x_ref[at, cols].astype(jnp.float32) * scale * g_ref[:, cols]).astype(jnp.bfloat16)
        return carry

    lax.fori_loop(0, x_ref.shape[0] // sub, piece, 0)


def normalize_some(x, norm_gain, start, rows):
    dim = x.shape[1]
    step = 64
    return pl.pallas_call(
        normalize_rows,
        grid=(rows // step,),
        in_specs=[pl.BlockSpec((step, dim), lambda i: (start // step + i, 0)), pl.BlockSpec((1, dim), lambda i: (0, 0))],
        out_specs=pl.BlockSpec((step, dim), lambda i: (i, 0)),
        out_shape=jax.ShapeDtypeStruct((rows, dim), jnp.bfloat16),
        compiler_params=pltpu.CompilerParams(vmem_limit_bytes=VMEM),
        cost_estimate=pl.CostEstimate(flops=8 * rows * dim, bytes_accessed=4 * rows * dim, transcendentals=rows),
        name="normalize_some",
    )(x, norm_gain)


def normalize_all(x, norm_gain, chunks, early):
    block, dim = x.shape
    step = NORM_ROWS
    starts = [sum(chunks[:i]) for i in range(len(chunks))]

    def body(x_ref, g_ref, *refs):
        outs, (held, sem) = refs[:-2], refs[-2:]
        b = pl.program_id(0)
        slot = lax.rem(b, 2)

        def copies(b, slot, do):
            do(pltpu.make_async_copy(held.at[slot], outs[0].at[pl.ds(b * step, step)], sem.at[slot, 0]))
            for k in range(block // step):

                @pl.when(b == k)
                def _(k=k):
                    count = 1
                    for i in range(early, len(chunks)):
                        low, high = max(k * step, starts[i]), min((k + 1) * step, starts[i] + chunks[i])
                        if low < high:
                            src = held.at[slot, pl.ds(low - k * step, high - low)]
                            dst = outs[1 + i - early].at[pl.ds(low - starts[i], high - low)]
                            do(pltpu.make_async_copy(src, dst, sem.at[slot, count]))
                            count += 1

        pl.when(b >= 2)(lambda: copies(b - 2, slot, lambda c: c.wait()))
        normalize_rows(x_ref, g_ref, held.at[slot])
        copies(b, slot, lambda c: c.start())

        @pl.when(b == block // step - 1)
        def _():
            copies(b - 1, 1 - slot, lambda c: c.wait())
            copies(b, slot, lambda c: c.wait())

    return pl.pallas_call(
        body,
        grid=(block // step,),
        in_specs=[pl.BlockSpec((step, dim), lambda i: (i, 0)), pl.BlockSpec((1, dim), lambda i: (0, 0))],
        out_specs=[pl.BlockSpec(memory_space=pl.ANY)] * (1 + len(chunks) - early),
        out_shape=[jax.ShapeDtypeStruct((rows, dim), jnp.bfloat16) for rows in (block,) + chunks[early:]],
        scratch_shapes=[pltpu.VMEM((2, step, dim), jnp.bfloat16), pltpu.SemaphoreType.DMA((2, 4))],
        compiler_params=pltpu.CompilerParams(vmem_limit_bytes=VMEM),
        cost_estimate=pl.CostEstimate(flops=8 * block * dim, bytes_accessed=6 * block * dim, transcendentals=block),
        name="normalize_all",
    )(x, norm_gain)


def join_weights(*weights):
    dim = weights[0].shape[0]
    step, sub = 512, 64
    steps = dim // step

    def body(a_ref, b_ref, c_ref, w_ref, held, flat, sem):
        def fetch(i, do):
            slot = lax.rem(i, 2)
            for index, ref in enumerate((a_ref, b_ref, c_ref)):
                src = ref.at[pl.ds(pl.multiple_of(i * step, step), step)]
                do(pltpu.make_async_copy(src, held.at[slot, index], sem.at[slot, index]))

        def block(i, carry):
            pl.when(i + 1 < steps)(lambda: fetch(i + 1, lambda copy: copy.start()))
            fetch(i, lambda copy: copy.wait())
            slot = lax.rem(i, 2)

            def some(k, carry):
                at = pl.ds(pl.multiple_of(k * sub, sub), sub)
                to = pl.ds(pl.multiple_of(i * step + k * sub, sub), sub)
                for index in range(3):
                    flat[index] = held[slot, index, at].astype(jnp.float32).reshape(sub * HEADS, HEAD_DIM)
                for index in range(3):
                    for head in range(HEADS):
                        part = flat[index, pl.ds(head, sub, stride=HEADS), :]
                        lanes = slice(head % SIDES * HEAD_DIM, (head % SIDES + 1) * HEAD_DIM)
                        w_ref[index * PIECES + head // SIDES, to, lanes] = part.astype(jnp.bfloat16)
                return carry

            return lax.fori_loop(0, step // sub, some, carry)

        fetch(0, lambda copy: copy.start())
        lax.fori_loop(0, steps, block, 0)

    return pl.pallas_call(
        body,
        in_specs=[pl.BlockSpec(memory_space=pl.ANY)] * 3,
        out_specs=pl.BlockSpec(memory_space=pltpu.VMEM),
        out_shape=pltpu.VMEM((3 * PIECES, dim, PIECE), jnp.bfloat16),
        scratch_shapes=[
            pltpu.VMEM((2, 3, step, HEADS, HEAD_DIM), jnp.bfloat16),
            pltpu.VMEM((3, sub * HEADS, HEAD_DIM), jnp.float32),
            pltpu.SemaphoreType.DMA((2, 3)),
        ],
        compiler_params=pltpu.CompilerParams(vmem_limit_bytes=JOIN_VMEM),
        cost_estimate=pl.CostEstimate(flops=6 * dim * COLS, bytes_accessed=6 * dim * COLS, transcendentals=0),
        name="join_weights",
    )(*weights)


def project(parts, w, owners, outs, tokens):
    arrays = [p[0] for p in parts]
    dim = w.shape[1]
    sizes = [p[1] for p in parts]
    offsets = [sum(sizes[:i]) for i in range(len(sizes))]
    rows = sum(sizes)
    blocks = arrays[0].shape[0] // sizes[0]
    steps = 3 * blocks
    slots = min(blocks, 2)
    quarter = rows // PIECES

    def body(owners_ref, *refs):
        n_hbm, w_ref = refs[: len(parts)], refs[len(parts)]
        q_out, k_out, v_out, n_buf, total, stage, n_sem, o_sem = refs[-8:]

        def fetch(b, do):
            slot = lax.rem(b, slots)
            for i, size in enumerate(sizes):
                src = n_hbm[i].at[pl.ds(pl.multiple_of(b * size, size), size)]
                do(pltpu.make_async_copy(src, n_buf.at[slot, pl.ds(offsets[i], size)], n_sem.at[slot, i]))

        def store(s, do):
            b, j = s // 3, lax.rem(s, 3)
            slot = lax.rem(s, 2)
            for index, out in enumerate((q_out, k_out, v_out)):

                @pl.when(j == index)
                def _(out=out):
                    for i, (_, size, which, start) in enumerate(parts):
                        first = owners_ref[which] * (tokens // 4) + start + b * size
                        src = stage.at[slot, pl.ds(offsets[i], size)]
                        do(pltpu.make_async_copy(src, out.at[pl.ds(first, size)], o_sem.at[slot, i]))

        def emit(slot, start, size):
            src = pl.ds(pl.multiple_of(start * HEADS, size * HEADS), size * HEADS)
            got = total[slot, src, :].reshape(size, HEADS, HEAD_DIM).astype(jnp.bfloat16)
            stage[slot, pl.ds(pl.multiple_of(start, size), size)] = got

        def begin(copy):
            copy.start()

        def end(copy):
            copy.wait()

        fetch(0, begin)

        def step(s, carry):
            b, j = s // 3, lax.rem(s, 3)
            slot = lax.rem(s, 2)
            pl.when(s >= 3)(lambda: store(s - 3, end))

            @pl.when(j == 0)
            def _():
                fetch(b, end)
                if blocks > 1:
                    pl.when(b + 1 < blocks)(lambda: fetch(b + 1, begin))

            def part(i, carry):
                emit(1 - slot, i * quarter, quarter)
                got = jnp.dot(n_buf[lax.rem(b, slots)], w_ref[j * PIECES + i], preferred_element_type=jnp.float32)
                for side in range(SIDES):
                    total[slot, pl.ds(SIDES * i + side, rows, stride=HEADS), :] = got[:, side * HEAD_DIM : (side + 1) * HEAD_DIM]
                return carry

            lax.fori_loop(0, PIECES, part, 0)
            pl.when(s >= 1)(lambda: store(s - 1, begin))
            return carry

        lax.fori_loop(0, steps, step, 0)
        last = steps - 1
        store(last - 2, end)
        lax.fori_loop(0, PIECES, lambda i, carry: (emit(last % 2, i * quarter, quarter), carry)[1], 0)
        store(last, begin)
        store(last - 1, end)
        store(last, end)

    return pl.pallas_call(
        body,
        in_specs=[pl.BlockSpec(memory_space=pltpu.SMEM)]
        + [pl.BlockSpec(memory_space=pl.ANY)] * len(parts)
        + [pl.BlockSpec(memory_space=pltpu.VMEM)]
        + [pl.BlockSpec(memory_space=pl.ANY)] * len(outs),
        out_specs=[pl.BlockSpec(memory_space=pl.ANY)] * 3,
        out_shape=[jax.ShapeDtypeStruct((tokens, HEADS, HEAD_DIM), jnp.bfloat16)] * 3,
        scratch_shapes=[
            pltpu.VMEM((slots, rows, dim), jnp.bfloat16),
            pltpu.VMEM((2, rows * HEADS, HEAD_DIM), jnp.float32),
            pltpu.VMEM((2, rows, HEADS, HEAD_DIM), jnp.bfloat16),
            pltpu.SemaphoreType.DMA((slots, len(parts))),
            pltpu.SemaphoreType.DMA((2, len(parts))),
        ],
        input_output_aliases={len(parts) + 2 + i: i for i in range(len(outs))},
        compiler_params=pltpu.CompilerParams(vmem_limit_bytes=PROJECT_VMEM),
        cost_estimate=pl.CostEstimate(
            flops=6 * blocks * rows * dim * COLS,
            bytes_accessed=2 * blocks * (rows * dim + 3 * rows * COLS),
            transcendentals=0,
        ),
        name="project",
    )(owners, *arrays, pltpu.with_memory_space_constraint(w, pltpu.VMEM), *outs)


def solution(mesh):
    across = [(0, 2), (1, 3), (2, 0), (3, 1)]
    beside = [(0, 1), (1, 0), (2, 3), (3, 2)]

    def inner(hidden_blk, norm_gain, wq_local, wk_local, wv_local):
        block, dim = hidden_blk.shape
        tokens = 4 * block
        me = lax.axis_index("tp").astype(jnp.int32)
        owners = me ^ jnp.arange(4, dtype=jnp.int32)
        starts = [sum(CHUNKS[:i]) for i in range(len(CHUNKS))]

        gain = norm_gain.reshape(1, dim)
        near = []
        for i in range(EARLY):
            m = normalize_some(hidden_blk, gain, starts[i], CHUNKS[i])
            near.append(lax.ppermute(m, "tp", across))
        own, *rest = normalize_all(hidden_blk, gain, CHUNKS, EARLY)
        for m in rest:
            near.append(lax.ppermute(m, "tp", across))
        paired = lax.ppermute(own, "tp", beside)
        w = join_weights(wq_local, wk_local, wv_local)

        far = {}

        def arrive(outs, *chunks):
            got = lax.optimization_barrier((tuple(near[i] for i in chunks), tuple(outs)))
            for i, a in zip(chunks, got[0]):
                near[i] = a
                far[i] = lax.ppermute(a, "tp", beside)
            return got[1]

        outs = project([(own, BIG, 0, 0)], w, owners, (), tokens)
        outs = arrive(outs, 0, 1, 2)
        outs = project([(paired, BIG, 1, 0)], w, owners, outs, tokens)
        outs = arrive(outs, 3)
        before = {5: (5,), 6: (6,), 7: (7,), 8: (8,), 9: (9, 10)}
        after = {2: (4,)}
        for group in ((0, 1), (2,), (3,), (4,), (5,), (6,), (7,), (8,), (9, 10)):
            for i in before.get(group[0], ()):
                outs = arrive(outs, i)
            parts = [(near[i], CHUNKS[i], 2, starts[i]) for i in group] + [(far[i], CHUNKS[i], 3, starts[i]) for i in group]
            outs = project(parts, w, owners, outs, tokens)
            for i in after.get(group[0], ()):
                outs = arrive(outs, i)
        return tuple(outs)

    row_spec = P(("dp", "tp"), None)
    head_spec = P(None, "tp", None)
    out_spec = P("dp", "tp", None)
    return jax.shard_map(inner, mesh=mesh, in_specs=(row_spec, P(None), head_spec, head_spec, head_spec), out_specs=(out_spec, out_spec, out_spec), check_vma=False)
```

```python
import jax
import jax.numpy as jnp
from jax import lax
from jax.experimental import pallas as pl
from jax.experimental.pallas import tpu as pltpu
from jax.sharding import PartitionSpec as P


HEADS = 8
HEAD_DIM = 128
COLS = HEADS * HEAD_DIM
SIDES = 4
PIECE = SIDES * HEAD_DIM
PIECES = COLS // PIECE
MIB = 1024 * 1024
VMEM = 48 * MIB
PROJECT_VMEM = 24 * MIB
JOIN_VMEM = 24 * MIB

CHUNKS = (64, 192, 256, 256, 256, 256, 256, 240, 128, 80, 64)
EARLY = 2
BIG = 512
NORM_ROWS = 128


def normalize_piece(x_ref, g_ref, n_ref, at):
    lanes = 128
    dim = x_ref.shape[1]
    squares = [jnp.zeros((at.size, lanes), jnp.float32) for _ in range(2)]
    for k in range(dim // lanes):
        v = x_ref[at, k * lanes : (k + 1) * lanes].astype(jnp.float32)
        squares[k % 2] += v * v
    mean = jnp.sum(squares[0] + squares[1], axis=-1, keepdims=True) / dim
    scale = jnp.broadcast_to(lax.rsqrt(mean + 1e-6), (at.size, lanes))
    for k in range(dim // lanes):
        cols = slice(k * lanes, (k + 1) * lanes)
        n_ref[at, cols] = (x_ref[at, cols].astype(jnp.float32) * scale * g_ref[:, cols]).astype(jnp.bfloat16)


def normalize_rows(x_ref, g_ref, n_ref):
    sub = 32

    def piece(i, carry):
        normalize_piece(x_ref, g_ref, n_ref, pl.ds(pl.multiple_of(i * sub, sub), sub))
        return carry

    lax.fori_loop(0, x_ref.shape[0] // sub, piece, 0)


def normalize_first(x, norm_gain, rows):
    dim = x.shape[1]
    sub = 32

    def body(x_hbm, g_hbm, n_ref, x_buf, g_buf, sem):
        gain = pltpu.make_async_copy(g_hbm, g_buf, sem.at[0])
        pieces = [pl.ds(i * sub, sub) for i in range(rows // sub)]
        copies = [pltpu.make_async_copy(x_hbm.at[at], x_buf.at[at], sem.at[1 + i]) for i, at in enumerate(pieces)]
        for copy in [gain] + copies:
            copy.start()
        gain.wait()
        for at, copy in zip(pieces, copies):
            copy.wait()
            normalize_piece(x_buf, g_buf, n_ref, at)

    return pl.pallas_call(
        body,
        in_specs=[pl.BlockSpec(memory_space=pl.ANY)] * 2,
        out_specs=pl.BlockSpec(memory_space=pltpu.VMEM),
        out_shape=pltpu.VMEM((rows, dim), jnp.bfloat16),
        scratch_shapes=[
            pltpu.VMEM((rows, dim), jnp.bfloat16),
            pltpu.VMEM((1, dim), jnp.float32),
            pltpu.SemaphoreType.DMA((1 + rows // sub,)),
        ],
        compiler_params=pltpu.CompilerParams(vmem_limit_bytes=VMEM),
        cost_estimate=pl.CostEstimate(flops=8 * rows * dim, bytes_accessed=2 * rows * dim, transcendentals=rows),
        name="normalize_first",
    )(x, norm_gain)


def normalize_some(x, norm_gain, start, rows):
    dim = x.shape[1]
    step = 64
    return pl.pallas_call(
        normalize_rows,
        grid=(rows // step,),
        in_specs=[pl.BlockSpec((step, dim), lambda i: (start // step + i, 0)), pl.BlockSpec((1, dim), lambda i: (0, 0))],
        out_specs=pl.BlockSpec((step, dim), lambda i: (i, 0)),
        out_shape=jax.ShapeDtypeStruct((rows, dim), jnp.bfloat16),
        compiler_params=pltpu.CompilerParams(vmem_limit_bytes=VMEM),
        cost_estimate=pl.CostEstimate(flops=8 * rows * dim, bytes_accessed=4 * rows * dim, transcendentals=rows),
        name="normalize_some",
    )(x, norm_gain)


def normalize_all(x, norm_gain, chunks, early):
    block, dim = x.shape
    step = NORM_ROWS
    starts = [sum(chunks[:i]) for i in range(len(chunks))]

    def body(x_ref, g_ref, *refs):
        outs, (held, sem) = refs[:-2], refs[-2:]
        b = pl.program_id(0)
        slot = lax.rem(b, 2)

        def copies(b, slot, do):
            do(pltpu.make_async_copy(held.at[slot], outs[0].at[pl.ds(b * step, step)], sem.at[slot, 0]))
            for k in range(block // step):

                @pl.when(b == k)
                def _(k=k):
                    count = 1
                    for i in range(early, len(chunks)):
                        low, high = max(k * step, starts[i]), min((k + 1) * step, starts[i] + chunks[i])
                        if low < high:
                            src = held.at[slot, pl.ds(low - k * step, high - low)]
                            dst = outs[1 + i - early].at[pl.ds(low - starts[i], high - low)]
                            do(pltpu.make_async_copy(src, dst, sem.at[slot, count]))
                            count += 1

        pl.when(b >= 2)(lambda: copies(b - 2, slot, lambda c: c.wait()))
        normalize_rows(x_ref, g_ref, held.at[slot])
        copies(b, slot, lambda c: c.start())

        @pl.when(b == block // step - 1)
        def _():
            copies(b - 1, 1 - slot, lambda c: c.wait())
            copies(b, slot, lambda c: c.wait())

    return pl.pallas_call(
        body,
        grid=(block // step,),
        in_specs=[pl.BlockSpec((step, dim), lambda i: (i, 0)), pl.BlockSpec((1, dim), lambda i: (0, 0))],
        out_specs=[pl.BlockSpec(memory_space=pl.ANY)] * (1 + len(chunks) - early),
        out_shape=[jax.ShapeDtypeStruct((rows, dim), jnp.bfloat16) for rows in (block,) + chunks[early:]],
        scratch_shapes=[pltpu.VMEM((2, step, dim), jnp.bfloat16), pltpu.SemaphoreType.DMA((2, 4))],
        compiler_params=pltpu.CompilerParams(vmem_limit_bytes=VMEM),
        cost_estimate=pl.CostEstimate(flops=8 * block * dim, bytes_accessed=6 * block * dim, transcendentals=block),
        name="normalize_all",
    )(x, norm_gain)


def join_weights(*weights):
    dim = weights[0].shape[0]
    step, sub = 512, 64
    steps = dim // step

    def body(a_ref, b_ref, c_ref, w_ref, held, flat, sem):
        def fetch(i, do):
            slot = lax.rem(i, 2)
            for index, ref in enumerate((a_ref, b_ref, c_ref)):
                src = ref.at[pl.ds(pl.multiple_of(i * step, step), step)]
                do(pltpu.make_async_copy(src, held.at[slot, index], sem.at[slot, index]))

        def block(i, carry):
            pl.when(i + 1 < steps)(lambda: fetch(i + 1, lambda copy: copy.start()))
            fetch(i, lambda copy: copy.wait())
            slot = lax.rem(i, 2)

            def some(k, carry):
                at = pl.ds(pl.multiple_of(k * sub, sub), sub)
                to = pl.ds(pl.multiple_of(i * step + k * sub, sub), sub)
                for index in range(3):
                    flat[index] = held[slot, index, at].astype(jnp.float32).reshape(sub * HEADS, HEAD_DIM)
                for index in range(3):
                    for head in range(HEADS):
                        part = flat[index, pl.ds(head, sub, stride=HEADS), :]
                        lanes = slice(head % SIDES * HEAD_DIM, (head % SIDES + 1) * HEAD_DIM)
                        w_ref[index * PIECES + head // SIDES, to, lanes] = part.astype(jnp.bfloat16)
                return carry

            return lax.fori_loop(0, step // sub, some, carry)

        fetch(0, lambda copy: copy.start())
        lax.fori_loop(0, steps, block, 0)

    return pl.pallas_call(
        body,
        in_specs=[pl.BlockSpec(memory_space=pl.ANY)] * 3,
        out_specs=pl.BlockSpec(memory_space=pltpu.VMEM),
        out_shape=pltpu.VMEM((3 * PIECES, dim, PIECE), jnp.bfloat16),
        scratch_shapes=[
            pltpu.VMEM((2, 3, step, HEADS, HEAD_DIM), jnp.bfloat16),
            pltpu.VMEM((3, sub * HEADS, HEAD_DIM), jnp.float32),
            pltpu.SemaphoreType.DMA((2, 3)),
        ],
        compiler_params=pltpu.CompilerParams(vmem_limit_bytes=JOIN_VMEM),
        cost_estimate=pl.CostEstimate(flops=6 * dim * COLS, bytes_accessed=6 * dim * COLS, transcendentals=0),
        name="join_weights",
    )(*weights)


def to_vmem(n):
    def body(n_ref, out_ref, sem):
        pltpu.make_async_copy(n_ref, out_ref, sem).start()
        pltpu.make_async_copy(n_ref, out_ref, sem).wait()

    return pl.pallas_call(
        body,
        in_specs=[pl.BlockSpec(memory_space=pl.ANY)],
        out_specs=pl.BlockSpec(memory_space=pltpu.VMEM),
        out_shape=pltpu.VMEM(n.shape, n.dtype),
        scratch_shapes=[pltpu.SemaphoreType.DMA],
        compiler_params=pltpu.CompilerParams(vmem_limit_bytes=MIB),
        cost_estimate=pl.CostEstimate(flops=n.size, bytes_accessed=4 * n.size, transcendentals=0),
        name="to_vmem",
    )(n)


def project(parts, w, owners, outs, tokens, resident=False):
    arrays = [pltpu.with_memory_space_constraint(p[0], pltpu.VMEM) if resident else p[0] for p in parts]
    dim = w.shape[1]
    sizes = [p[1] for p in parts]
    offsets = [sum(sizes[:i]) for i in range(len(sizes))]
    rows = sum(sizes)
    blocks = arrays[0].shape[0] // sizes[0]
    steps = 3 * blocks
    slots = min(blocks, 2)
    quarter = rows // PIECES

    def body(owners_ref, *refs):
        n_hbm, w_ref = refs[: len(parts)], refs[len(parts)]
        q_out, k_out, v_out, n_buf, total, stage, n_sem, o_sem = refs[-8:]

        def fetch(b, do):
            if resident:
                if do is end:
                    for i, size in enumerate(sizes):
                        n_buf[0, offsets[i] : offsets[i] + size, :] = n_hbm[i][...]
                return
            slot = lax.rem(b, slots)
            for i, size in enumerate(sizes):
                src = n_hbm[i].at[pl.ds(pl.multiple_of(b * size, size), size)]
                do(pltpu.make_async_copy(src, n_buf.at[slot, pl.ds(offsets[i], size)], n_sem.at[slot, i]))

        def store(s, do):
            b, j = s // 3, lax.rem(s, 3)
            slot = lax.rem(s, 2)
            for index, out in enumerate((q_out, k_out, v_out)):

                @pl.when(j == index)
                def _(out=out):
                    for i, (_, size, which, start) in enumerate(parts):
                        first = owners_ref[which] * (tokens // 4) + start + b * size
                        src = stage.at[slot, pl.ds(offsets[i], size)]
                        do(pltpu.make_async_copy(src, out.at[pl.ds(first, size)], o_sem.at[slot, i]))

        def emit(slot, start, size):
            src = pl.ds(pl.multiple_of(start * HEADS, size * HEADS), size * HEADS)
            got = total[slot, src, :].reshape(size, HEADS, HEAD_DIM).astype(jnp.bfloat16)
            stage[slot, pl.ds(pl.multiple_of(start, size), size)] = got

        def begin(copy):
            copy.start()

        def end(copy):
            copy.wait()

        fetch(0, begin)

        def step(s, carry):
            b, j = s // 3, lax.rem(s, 3)
            slot = lax.rem(s, 2)
            pl.when(s >= 3)(lambda: store(s - 3, end))

            @pl.when(j == 0)
            def _():
                fetch(b, end)
                if blocks > 1:
                    pl.when(b + 1 < blocks)(lambda: fetch(b + 1, begin))

            def part(i, carry):
                emit(1 - slot, i * quarter, quarter)
                got = jnp.dot(n_buf[lax.rem(b, slots)], w_ref[j * PIECES + i], preferred_element_type=jnp.float32)
                for side in range(SIDES):
                    total[slot, pl.ds(SIDES * i + side, rows, stride=HEADS), :] = got[:, side * HEAD_DIM : (side + 1) * HEAD_DIM]
                return carry

            lax.fori_loop(0, PIECES, part, 0)
            pl.when(s >= 1)(lambda: store(s - 1, begin))
            return carry

        lax.fori_loop(0, steps, step, 0)
        last = steps - 1
        store(last - 2, end)
        lax.fori_loop(0, PIECES, lambda i, carry: (emit(last % 2, i * quarter, quarter), carry)[1], 0)
        store(last, begin)
        store(last - 1, end)
        store(last, end)

    return pl.pallas_call(
        body,
        in_specs=[pl.BlockSpec(memory_space=pltpu.SMEM)]
        + [pl.BlockSpec(memory_space=pltpu.VMEM if resident else pl.ANY)] * len(parts)
        + [pl.BlockSpec(memory_space=pltpu.VMEM)]
        + [pl.BlockSpec(memory_space=pl.ANY)] * len(outs),
        out_specs=[pl.BlockSpec(memory_space=pl.ANY)] * 3,
        out_shape=[jax.ShapeDtypeStruct((tokens, HEADS, HEAD_DIM), jnp.bfloat16)] * 3,
        scratch_shapes=[
            pltpu.VMEM((slots, rows, dim), jnp.bfloat16),
            pltpu.VMEM((2, rows * HEADS, HEAD_DIM), jnp.float32),
            pltpu.VMEM((2, rows, HEADS, HEAD_DIM), jnp.bfloat16),
            pltpu.SemaphoreType.DMA((slots, len(parts))),
            pltpu.SemaphoreType.DMA((2, len(parts))),
        ],
        input_output_aliases={len(parts) + 2 + i: i for i in range(len(outs))},
        compiler_params=pltpu.CompilerParams(vmem_limit_bytes=PROJECT_VMEM),
        cost_estimate=pl.CostEstimate(
            flops=6 * blocks * rows * dim * COLS,
            bytes_accessed=2 * blocks * (rows * dim + 3 * rows * COLS),
            transcendentals=0,
        ),
        name="project",
    )(owners, *arrays, pltpu.with_memory_space_constraint(w, pltpu.VMEM), *outs)


def solution(mesh):
    across = [(0, 2), (1, 3), (2, 0), (3, 1)]
    beside = [(0, 1), (1, 0), (2, 3), (3, 2)]

    def inner(hidden_blk, norm_gain, wq_local, wk_local, wv_local):
        block, dim = hidden_blk.shape
        tokens = 4 * block
        me = lax.axis_index("tp").astype(jnp.int32)
        owners = me ^ jnp.arange(4, dtype=jnp.int32)
        starts = [sum(CHUNKS[:i]) for i in range(len(CHUNKS))]

        gain = pltpu.with_memory_space_constraint(norm_gain.reshape(1, dim), pltpu.HBM)
        near = []
        for i in range(EARLY):
            m = normalize_some(hidden_blk, gain, starts[i], CHUNKS[i]) if i else normalize_first(hidden_blk, gain, CHUNKS[i])
            near.append(lax.ppermute(m, "tp", across))
        own, *rest = normalize_all(hidden_blk, gain, CHUNKS, EARLY)
        for m in rest:
            near.append(lax.ppermute(m, "tp", across))
        paired = lax.ppermute(own, "tp", beside)
        w = join_weights(wq_local, wk_local, wv_local)

        far = {}

        def arrive(outs, *chunks):
            got = lax.optimization_barrier((tuple(near[i] for i in chunks), tuple(outs)))
            for i, a in zip(chunks, got[0]):
                near[i] = a
                far[i] = lax.ppermute(a, "tp", beside)
                if i == len(CHUNKS) - 1:
                    near[i] = to_vmem(a)
            return got[1]

        outs = project([(own, BIG, 0, 0)], w, owners, (), tokens)
        outs = arrive(outs, 0, 1, 2)
        outs = project([(paired, BIG, 1, 0)], w, owners, outs, tokens)
        outs = arrive(outs, 3)
        before = {5: (5,), 6: (6,), 7: (7,), 8: (8,), 9: (9,), 10: (10,)}
        after = {2: (4,)}
        for group in ((0, 1), (2,), (3,), (4,), (5,), (6,), (7,), (8,), (9,), (10,)):
            for i in before.get(group[0], ()):
                outs = arrive(outs, i)
            parts = [(near[i], CHUNKS[i], 2, starts[i]) for i in group] + [(far[i], CHUNKS[i], 3, starts[i]) for i in group]
            outs = project(parts, w, owners, outs, tokens, resident=group[-1] == len(CHUNKS) - 1)
            for i in after.get(group[0], ()):
                outs = arrive(outs, i)
        return tuple(outs)

    row_spec = P(("dp", "tp"), None)
    head_spec = P(None, "tp", None)
    out_spec = P("dp", "tp", None)
    return jax.shard_map(inner, mesh=mesh, in_specs=(row_spec, P(None), head_spec, head_spec, head_spec), out_specs=(out_spec, out_spec, out_spec), check_vma=False)
```

```python
import jax
import jax.numpy as jnp
from jax import lax
from jax.experimental import pallas as pl
from jax.experimental.pallas import tpu as pltpu
from jax.sharding import PartitionSpec as P


HEADS = 8
HEAD_DIM = 128
COLS = HEADS * HEAD_DIM
SIDES = 4
PIECE = SIDES * HEAD_DIM
PIECES = COLS // PIECE
MIB = 1024 * 1024
VMEM = 48 * MIB
PROJECT_VMEM = 24 * MIB
JOIN_VMEM = 24 * MIB

CHUNKS = (64, 192, 256, 256, 256, 256, 256, 240, 128, 80, 64)
EARLY = 2
BIG = 512
NORM_ROWS = 128


def normalize_piece(x_ref, g_ref, n_ref, at):
    lanes = 128
    dim = x_ref.shape[1]
    squares = [jnp.zeros((at.size, lanes), jnp.float32) for _ in range(2)]
    for k in range(dim // lanes):
        v = x_ref[at, k * lanes : (k + 1) * lanes].astype(jnp.float32)
        squares[k % 2] += v * v
    mean = jnp.sum(squares[0] + squares[1], axis=-1, keepdims=True) / dim
    scale = jnp.broadcast_to(lax.rsqrt(mean + 1e-6), (at.size, lanes))
    for k in range(dim // lanes):
        cols = slice(k * lanes, (k + 1) * lanes)
        n_ref[at, cols] = (x_ref[at, cols].astype(jnp.float32) * scale * g_ref[:, cols]).astype(jnp.bfloat16)


def normalize_rows(x_ref, g_ref, n_ref):
    sub = 32

    def piece(i, carry):
        normalize_piece(x_ref, g_ref, n_ref, pl.ds(pl.multiple_of(i * sub, sub), sub))
        return carry

    lax.fori_loop(0, x_ref.shape[0] // sub, piece, 0)


def normalize_first(x, norm_gain, rows):
    dim = x.shape[1]
    sub = 32

    def body(x_hbm, g_hbm, n_ref, x_buf, g_buf, sem):
        gain = pltpu.make_async_copy(g_hbm, g_buf, sem.at[0])
        pieces = [pl.ds(i * sub, sub) for i in range(rows // sub)]
        copies = [pltpu.make_async_copy(x_hbm.at[at], x_buf.at[at], sem.at[1 + i]) for i, at in enumerate(pieces)]
        for copy in [gain] + copies:
            copy.start()
        gain.wait()
        for at, copy in zip(pieces, copies):
            copy.wait()
            normalize_piece(x_buf, g_buf, n_ref, at)

    return pl.pallas_call(
        body,
        in_specs=[pl.BlockSpec(memory_space=pl.ANY)] * 2,
        out_specs=pl.BlockSpec(memory_space=pltpu.VMEM),
        out_shape=pltpu.VMEM((rows, dim), jnp.bfloat16),
        scratch_shapes=[
            pltpu.VMEM((rows, dim), jnp.bfloat16),
            pltpu.VMEM((1, dim), jnp.float32),
            pltpu.SemaphoreType.DMA((1 + rows // sub,)),
        ],
        compiler_params=pltpu.CompilerParams(vmem_limit_bytes=VMEM),
        cost_estimate=pl.CostEstimate(flops=8 * rows * dim, bytes_accessed=2 * rows * dim, transcendentals=rows),
        name="normalize_first",
    )(x, norm_gain)


def normalize_some(x, norm_gain, start, rows):
    dim = x.shape[1]
    step = 64
    return pl.pallas_call(
        normalize_rows,
        grid=(rows // step,),
        in_specs=[pl.BlockSpec((step, dim), lambda i: (start // step + i, 0)), pl.BlockSpec((1, dim), lambda i: (0, 0))],
        out_specs=pl.BlockSpec((step, dim), lambda i: (i, 0)),
        out_shape=jax.ShapeDtypeStruct((rows, dim), jnp.bfloat16),
        compiler_params=pltpu.CompilerParams(vmem_limit_bytes=VMEM),
        cost_estimate=pl.CostEstimate(flops=8 * rows * dim, bytes_accessed=4 * rows * dim, transcendentals=rows),
        name="normalize_some",
    )(x, norm_gain)


def normalize_all(x, norm_gain, chunks, early):
    block, dim = x.shape
    step = NORM_ROWS
    starts = [sum(chunks[:i]) for i in range(len(chunks))]

    def body(x_ref, g_ref, *refs):
        outs, (held, sem) = refs[:-2], refs[-2:]
        b = pl.program_id(0)
        slot = lax.rem(b, 2)

        def copies(b, slot, do):
            do(pltpu.make_async_copy(held.at[slot], outs[0].at[pl.ds(b * step, step)], sem.at[slot, 0]))
            for k in range(block // step):

                @pl.when(b == k)
                def _(k=k):
                    count = 1
                    for i in range(early, len(chunks)):
                        low, high = max(k * step, starts[i]), min((k + 1) * step, starts[i] + chunks[i])
                        if low < high:
                            src = held.at[slot, pl.ds(low - k * step, high - low)]
                            dst = outs[1 + i - early].at[pl.ds(low - starts[i], high - low)]
                            do(pltpu.make_async_copy(src, dst, sem.at[slot, count]))
                            count += 1

        pl.when(b >= 2)(lambda: copies(b - 2, slot, lambda c: c.wait()))
        normalize_rows(x_ref, g_ref, held.at[slot])
        copies(b, slot, lambda c: c.start())

        @pl.when(b == block // step - 1)
        def _():
            copies(b - 1, 1 - slot, lambda c: c.wait())
            copies(b, slot, lambda c: c.wait())

    return pl.pallas_call(
        body,
        grid=(block // step,),
        in_specs=[pl.BlockSpec((step, dim), lambda i: (i, 0)), pl.BlockSpec((1, dim), lambda i: (0, 0))],
        out_specs=[pl.BlockSpec(memory_space=pl.ANY)] * (1 + len(chunks) - early),
        out_shape=[jax.ShapeDtypeStruct((rows, dim), jnp.bfloat16) for rows in (block,) + chunks[early:]],
        scratch_shapes=[pltpu.VMEM((2, step, dim), jnp.bfloat16), pltpu.SemaphoreType.DMA((2, 4))],
        compiler_params=pltpu.CompilerParams(vmem_limit_bytes=VMEM),
        cost_estimate=pl.CostEstimate(flops=8 * block * dim, bytes_accessed=6 * block * dim, transcendentals=block),
        name="normalize_all",
    )(x, norm_gain)


def join_weights(*weights):
    dim = weights[0].shape[0]
    step, sub = 512, 64
    steps = dim // step

    def body(a_ref, b_ref, c_ref, w_ref, held, flat, sem):
        def fetch(i, do):
            slot = lax.rem(i, 2)
            for index, ref in enumerate((a_ref, b_ref, c_ref)):
                src = ref.at[pl.ds(pl.multiple_of(i * step, step), step)]
                do(pltpu.make_async_copy(src, held.at[slot, index], sem.at[slot, index]))

        def block(i, carry):
            pl.when(i + 1 < steps)(lambda: fetch(i + 1, lambda copy: copy.start()))
            fetch(i, lambda copy: copy.wait())
            slot = lax.rem(i, 2)

            def some(k, carry):
                at = pl.ds(pl.multiple_of(k * sub, sub), sub)
                to = pl.ds(pl.multiple_of(i * step + k * sub, sub), sub)
                for index in range(3):
                    flat[index] = held[slot, index, at].astype(jnp.float32).reshape(sub * HEADS, HEAD_DIM)
                for index in range(3):
                    for head in range(HEADS):
                        part = flat[index, pl.ds(head, sub, stride=HEADS), :]
                        lanes = slice(head % SIDES * HEAD_DIM, (head % SIDES + 1) * HEAD_DIM)
                        w_ref[index * PIECES + head // SIDES, to, lanes] = part.astype(jnp.bfloat16)
                return carry

            return lax.fori_loop(0, step // sub, some, carry)

        fetch(0, lambda copy: copy.start())
        lax.fori_loop(0, steps, block, 0)

    return pl.pallas_call(
        body,
        in_specs=[pl.BlockSpec(memory_space=pl.ANY)] * 3,
        out_specs=pl.BlockSpec(memory_space=pltpu.VMEM),
        out_shape=pltpu.VMEM((3 * PIECES, dim, PIECE), jnp.bfloat16),
        scratch_shapes=[
            pltpu.VMEM((2, 3, step, HEADS, HEAD_DIM), jnp.bfloat16),
            pltpu.VMEM((3, sub * HEADS, HEAD_DIM), jnp.float32),
            pltpu.SemaphoreType.DMA((2, 3)),
        ],
        compiler_params=pltpu.CompilerParams(vmem_limit_bytes=JOIN_VMEM),
        cost_estimate=pl.CostEstimate(flops=6 * dim * COLS, bytes_accessed=6 * dim * COLS, transcendentals=0),
        name="join_weights",
    )(*weights)


def project(parts, w, owners, outs, tokens, resident=False):
    arrays = [pltpu.with_memory_space_constraint(p[0], pltpu.VMEM) if resident else p[0] for p in parts]
    dim = w.shape[1]
    sizes = [p[1] for p in parts]
    offsets = [sum(sizes[:i]) for i in range(len(sizes))]
    rows = sum(sizes)
    blocks = arrays[0].shape[0] // sizes[0]
    steps = 3 * blocks
    slots = min(blocks, 2)
    quarter = rows // PIECES

    def body(owners_ref, *refs):
        n_hbm, w_ref = refs[: len(parts)], refs[len(parts)]
        q_out, k_out, v_out, n_buf, total, stage, n_sem, o_sem = refs[-8:]

        def fetch(b, do):
            if resident:
                if do is end:
                    for i, size in enumerate(sizes):
                        n_buf[0, offsets[i] : offsets[i] + size, :] = n_hbm[i][...]
                return
            slot = lax.rem(b, slots)
            for i, size in enumerate(sizes):
                src = n_hbm[i].at[pl.ds(pl.multiple_of(b * size, size), size)]
                do(pltpu.make_async_copy(src, n_buf.at[slot, pl.ds(offsets[i], size)], n_sem.at[slot, i]))

        def store(s, do):
            b, j = s // 3, lax.rem(s, 3)
            slot = lax.rem(s, 2)
            for index, out in enumerate((q_out, k_out, v_out)):

                @pl.when(j == index)
                def _(out=out):
                    for i, (_, size, which, start) in enumerate(parts):
                        first = owners_ref[which] * (tokens // 4) + start + b * size
                        src = stage.at[slot, pl.ds(offsets[i], size)]
                        do(pltpu.make_async_copy(src, out.at[pl.ds(first, size)], o_sem.at[slot, i]))

        def emit(slot, start, size):
            src = pl.ds(pl.multiple_of(start * HEADS, size * HEADS), size * HEADS)
            got = total[slot, src, :].reshape(size, HEADS, HEAD_DIM).astype(jnp.bfloat16)
            stage[slot, pl.ds(pl.multiple_of(start, size), size)] = got

        def begin(copy):
            copy.start()

        def end(copy):
            copy.wait()

        fetch(0, begin)

        def step(s, carry):
            b, j = s // 3, lax.rem(s, 3)
            slot = lax.rem(s, 2)
            pl.when(s >= 3)(lambda: store(s - 3, end))

            @pl.when(j == 0)
            def _():
                fetch(b, end)
                if blocks > 1:
                    pl.when(b + 1 < blocks)(lambda: fetch(b + 1, begin))

            def part(i, carry):
                emit(1 - slot, i * quarter, quarter)
                got = jnp.dot(n_buf[lax.rem(b, slots)], w_ref[j * PIECES + i], preferred_element_type=jnp.float32)
                for side in range(SIDES):
                    total[slot, pl.ds(SIDES * i + side, rows, stride=HEADS), :] = got[:, side * HEAD_DIM : (side + 1) * HEAD_DIM]
                return carry

            lax.fori_loop(0, PIECES, part, 0)
            pl.when(s >= 1)(lambda: store(s - 1, begin))
            return carry

        lax.fori_loop(0, steps, step, 0)
        last = steps - 1
        store(last - 2, end)
        lax.fori_loop(0, PIECES, lambda i, carry: (emit(last % 2, i * quarter, quarter), carry)[1], 0)
        store(last, begin)
        store(last - 1, end)
        store(last, end)

    return pl.pallas_call(
        body,
        in_specs=[pl.BlockSpec(memory_space=pltpu.SMEM)]
        + [pl.BlockSpec(memory_space=pltpu.VMEM if resident else pl.ANY)] * len(parts)
        + [pl.BlockSpec(memory_space=pltpu.VMEM)]
        + [pl.BlockSpec(memory_space=pl.ANY)] * len(outs),
        out_specs=[pl.BlockSpec(memory_space=pl.ANY)] * 3,
        out_shape=[jax.ShapeDtypeStruct((tokens, HEADS, HEAD_DIM), jnp.bfloat16)] * 3,
        scratch_shapes=[
            pltpu.VMEM((slots, rows, dim), jnp.bfloat16),
            pltpu.VMEM((2, rows * HEADS, HEAD_DIM), jnp.float32),
            pltpu.VMEM((2, rows, HEADS, HEAD_DIM), jnp.bfloat16),
            pltpu.SemaphoreType.DMA((slots, len(parts))),
            pltpu.SemaphoreType.DMA((2, len(parts))),
        ],
        input_output_aliases={len(parts) + 2 + i: i for i in range(len(outs))},
        compiler_params=pltpu.CompilerParams(vmem_limit_bytes=PROJECT_VMEM),
        cost_estimate=pl.CostEstimate(
            flops=6 * blocks * rows * dim * COLS,
            bytes_accessed=2 * blocks * (rows * dim + 3 * rows * COLS),
            transcendentals=0,
        ),
        name="project",
    )(owners, *arrays, pltpu.with_memory_space_constraint(w, pltpu.VMEM), *outs)


def solution(mesh):
    across = [(0, 2), (1, 3), (2, 0), (3, 1)]
    beside = [(0, 1), (1, 0), (2, 3), (3, 2)]

    def inner(hidden_blk, norm_gain, wq_local, wk_local, wv_local):
        block, dim = hidden_blk.shape
        tokens = 4 * block
        me = lax.axis_index("tp").astype(jnp.int32)
        owners = me ^ jnp.arange(4, dtype=jnp.int32)
        starts = [sum(CHUNKS[:i]) for i in range(len(CHUNKS))]

        gain = pltpu.with_memory_space_constraint(norm_gain.reshape(1, dim), pltpu.HBM)
        near = []
        for i in range(EARLY):
            m = normalize_some(hidden_blk, gain, starts[i], CHUNKS[i]) if i else normalize_first(hidden_blk, gain, CHUNKS[i])
            near.append(lax.ppermute(m, "tp", across))
        own, *rest = normalize_all(hidden_blk, gain, CHUNKS, EARLY)
        for m in rest:
            near.append(lax.ppermute(m, "tp", across))
        paired = lax.ppermute(own, "tp", beside)
        w = join_weights(wq_local, wk_local, wv_local)

        far = {}

        def arrive(outs, *chunks):
            got = lax.optimization_barrier((tuple(near[i] for i in chunks), tuple(outs)))
            for i, a in zip(chunks, got[0]):
                near[i] = a
                far[i] = lax.ppermute(a, "tp", beside)
            return got[1]

        outs = project([(own, BIG, 0, 0)], w, owners, (), tokens)
        outs = arrive(outs, 0, 1, 2)
        outs = project([(paired, BIG, 1, 0)], w, owners, outs, tokens)
        outs = arrive(outs, 3)
        before = {5: (5,), 6: (6,), 7: (7,), 8: (8,), 9: (9,), 10: (10,)}
        after = {2: (4,)}
        for group in ((0, 1), (2,), (3,), (4,), (5,), (6,), (7,), (8,), (9,), (10,)):
            for i in before.get(group[0], ()):
                outs = arrive(outs, i)
            parts = [(near[i], CHUNKS[i], 2, starts[i]) for i in group] + [(far[i], CHUNKS[i], 3, starts[i]) for i in group]
            outs = project(parts, w, owners, outs, tokens, resident=group[-1] == len(CHUNKS) - 1)
            for i in after.get(group[0], ()):
                outs = arrive(outs, i)
        return tuple(outs)

    row_spec = P(("dp", "tp"), None)
    head_spec = P(None, "tp", None)
    out_spec = P("dp", "tp", None)
    return jax.shard_map(inner, mesh=mesh, in_specs=(row_spec, P(None), head_spec, head_spec, head_spec), out_specs=(out_spec, out_spec, out_spec), check_vma=False)
```
